32 devices in a mesh: inst: 4 (over x, core), shard: 8 (over z, y).
Axes of the slice: x: 2, y: 2, z: 4, core: 2. Of those that a mesh axis runs over, the one named last changes fastest.
Arguments:
- tokens: bfloat16 [2048, 5120], P(('inst', 'shard')), may hold values from -600 to 600
- norm_gain: float32 [5120], P(('inst', 'shard')), may hold values from 0.1 to 1.9
- master_qkv: float32 [5120, 7168], P(('inst', 'shard')), may hold values from -0.078125 to 0.078125
- qkv_bias: float32 [7168], P(('inst', 'shard')), may hold values from -3 to 3
Outputs:
- qkv_out: bfloat16 [32, 512, 896], P(('inst', 'shard'))
The draws below stay inside these ranges and needn't reach their ends.
All inputs are finite; a program needn't handle non-finite values.
Results may differ from the reference program's by a relative error of at most 0.0062.
Values may be sent and summed in bfloat16 or wider, within the bound.
A program may use at most 64 MiB of HBM per device.

```python
import jax
import jax.numpy as jnp
from jax import lax

D = 5120
QHEADS = 40
KVHEADS = 8
HEAD_DIM = 128
TP = 8
TOK_DEV = 64
QKVW = 7168
TOKENS = 2048
N_INST = 4
N_SHARD = 8


def draw_tokens(key, part):
    row_key, col_key, base_key = jax.random.split(key, 3)
    base = jax.random.truncated_normal(base_key, -4.0, 4.0, (TOKENS, D), jnp.float32)
    row_scale = jnp.power(10.0, jax.random.uniform(row_key, (TOKENS, 1), jnp.float32, 0.0, 1.0))
    col_scale = jnp.power(10.0, jax.random.uniform(col_key, (1, D), jnp.float32, 0.0, 1.0))
    return (base * row_scale * col_scale).astype(jnp.bfloat16)


def block_scale(stream_key, shape, cuts, smallest, largest):
    level = 1.0
    for position, shards_of in cuts:
        heights = jax.random.uniform(jax.random.fold_in(jax.random.fold_in(stream_key, 6), position), (shards_of,), jnp.float32, smallest / len(cuts), largest / len(cuts))
        level = level * jnp.repeat(jnp.exp(heights), shape[position] // shards_of).reshape((-1,) + (1,) * (len(shape) - 1 - position))
    return level


def scatter_about(stream_key, extent, scale, bound, cuts=(), dtype=jnp.bfloat16):
    entries = jax.random.normal(stream_key, extent, jnp.float32) * scale
    if len(cuts) > 0:
        entries = block_scale(stream_key, extent, cuts, -0.22, 0.18) * entries
    return jnp.clip(entries, min=-bound, max=bound).astype(dtype)


def setup_inputs(seed: int = 0) -> dict:
    key_of = jax.random.split(jax.random.key(seed), 5)
    tokens = draw_tokens(jax.random.fold_in(key_of[4], 71), 0)
    norm_gain = jnp.clip(1.0 + 0.18 * jax.random.normal(key_of[1], (D,), jnp.float32), 0.1, 1.9)
    master_qkv = scatter_about(key_of[2], (D, QKVW), D ** -0.5, 0.078125, ((0, 32),), jnp.float32)
    qkv_bias = scatter_about(key_of[3], (QKVW,), 0.5, 3.0, ((0, 32),), jnp.float32)
    return {"tokens": tokens, "norm_gain": norm_gain, "master_qkv": master_qkv, "qkv_bias": qkv_bias}


EPSILON = 1e-06

def rank_columns(matrix):
    query_cols = QHEADS * HEAD_DIM
    pair_cols = KVHEADS * HEAD_DIM
    leading = matrix.shape[:-1]
    query = matrix[..., :query_cols].reshape(leading + (TP, query_cols // TP))
    keys = matrix[..., query_cols:query_cols + pair_cols].reshape(leading + (TP, pair_cols // TP))
    values = matrix[..., query_cols + pair_cols:].reshape(leading + (TP, pair_cols // TP))
    return jnp.concatenate([query, keys, values], axis=-1)

def normalize(tokens, gain):
    floats = tokens.astype(jnp.float32)
    scale = lax.rsqrt(lax.optimization_barrier(jnp.mean(floats * floats, axis=-1, keepdims=True)) + EPSILON)
    return (floats * scale * gain.astype(jnp.float32)).astype(jnp.bfloat16)

def reference(tokens, norm_gain, master_qkv, qkv_bias):
    weights = master_qkv.astype(jnp.bfloat16)
    gain_low = norm_gain.astype(jnp.bfloat16)
    bias_low = qkv_bias.astype(jnp.bfloat16)
    normed = normalize(tokens, gain_low)
    rank_width = QKVW // TP
    flat_weights = rank_columns(weights).reshape(D, TP * rank_width)
    flat_bias = rank_columns(bias_low).reshape(TP * rank_width).astype(jnp.float32)
    group_tokens = TP * TOK_DEV
    groups = normed.reshape(TOKENS // group_tokens, group_tokens, D)

    def project(group_rows):
        product = jnp.dot(group_rows, flat_weights, preferred_element_type=jnp.float32) + flat_bias
        shaped = product.astype(jnp.bfloat16).reshape(group_tokens, TP, rank_width)
        return jnp.transpose(shaped, (1, 0, 2))
    outputs = lax.map(project, groups)
    return outputs.reshape(N_INST * N_SHARD, group_tokens, rank_width)
```

```python
import functools

import jax
import jax.numpy as jnp
from jax import lax
from jax.experimental import pallas as pl
from jax.experimental.pallas import tpu as pltpu
from jax.sharding import PartitionSpec as P

QHEADS = 40
KVHEADS = 8
HEAD_DIM = 128
TP = 8


EPSILON = 1e-06
MESH = pl.DeviceIdType.MESH
LANES = 128
TOKEN_PIECES = 2


def partner_2(value, axis, distance):
    mask = 2**distance
    pairs = [(source, source ^ mask) for source in range(lax.axis_size(axis))]
    return lax.ppermute(value, axis, pairs)


def rank_columns(matrix):
    query_cols = QHEADS * HEAD_DIM
    pair_cols = KVHEADS * HEAD_DIM
    leading = matrix.shape[:-1]
    query = matrix[..., :query_cols].reshape(leading + (TP, query_cols // TP))
    keys = matrix[..., query_cols : query_cols + pair_cols].reshape(leading + (TP, pair_cols // TP))
    values = matrix[..., query_cols + pair_cols :].reshape(leading + (TP, pair_cols // TP))
    return jnp.concatenate([query, keys, values], axis=-1)


def normalize(tokens, gain):
    floats = tokens.astype(jnp.float32)
    scale = lax.rsqrt(jnp.mean(floats * floats, axis=-1, keepdims=True) + EPSILON)
    return (floats * scale * gain.astype(jnp.float32)).astype(jnp.bfloat16)


def general_device(tokens, norm_gain, master_qkv, qkv_bias):
    shard_count = lax.axis_size("shard")
    local_rows = master_qkv.shape[0]
    rank_width = master_qkv.shape[1] // TP
    gain_full, bias_full = (
        lax.all_gather(norm_gain.astype(jnp.bfloat16), ("inst", "shard"), axis=0, tiled=True),
        lax.all_gather(qkv_bias.astype(jnp.bfloat16), ("inst", "shard"), axis=0, tiled=True),
    )
    normed = normalize(tokens, gain_full)
    shard_pos = lax.axis_index("shard")
    rank_index = shard_pos % TP
    bit_count = TP.bit_length() - 1
    bit_order = list(range(bit_count))
    group_rows = normed
    for bit_pos in bit_order:
        partner = partner_2(group_rows, "shard", bit_pos)
        lower = jnp.bitwise_and(jnp.right_shift(shard_pos, bit_pos), 1) == 0
        group_rows = jnp.where(
            lower,
            jnp.concatenate([group_rows, partner], 0),
            jnp.concatenate([partner, group_rows], 0),
        )
    copies = shard_count // TP
    inst_block = shard_count * local_rows
    rows_low = master_qkv.astype(jnp.bfloat16)
    ranked = jnp.transpose(rank_columns(rows_low), (1, 0, 2))
    spread = jnp.broadcast_to(ranked[None], (copies,) + ranked.shape)
    outgoing = spread.reshape(shard_count, rows_low.shape[0], rank_width)
    arrived = lax.all_to_all(outgoing, "shard", split_axis=0, concat_axis=0, tiled=True).reshape(
        inst_block, rank_width
    )
    product = jnp.dot(
        group_rows,
        lax.all_gather(arrived, "inst", axis=0, tiled=True),
        preferred_element_type=jnp.float32,
    )
    bias_ranks = rank_columns(bias_full)
    bias_mine = lax.dynamic_index_in_dim(bias_ranks, rank_index, 0, keepdims=False)
    result = (product + bias_mine.astype(jnp.float32)).astype(jnp.bfloat16)
    return result[None]


def kernel(
    dims,
    tok_ref,
    gain_ref,
    w_ref,
    bias_ref,
    out_ref,
    tbuf,
    wbuf,
    wsend,
    bbuf,
    scale_ref,
    t_recv,
    t_send,
    w_recv,
    a_send,
    x_send,
    d_send,
    b_recv,
    b_send,
):
    inst_count, shard_count, group = dims
    devices = inst_count * shard_count
    line = shard_count // 2
    inst = lax.axis_index("inst")
    me = lax.axis_index("shard")
    z = me // 2
    y = lax.rem(me, 2)
    flat = inst * shard_count + me
    core_peer = inst + 1 - 2 * lax.rem(inst, 2)
    x_peer = lax.rem(inst + 2, inst_count)
    y_peer = z * 2 + 1 - y
    rows = w_ref.shape[0]
    width = wsend.shape[2]
    pieces = TOKEN_PIECES
    piece_rows = tok_ref.shape[0] // pieces

    def mate(k):
        dy, dz = k % 2, k // 2
        zz = z if dz == 0 else (z + 1 - 2 * lax.rem(z, 2), lax.rem(z + 2, line), line - 1 - z)[dz - 1]
        return zz * 2 + lax.rem(y + dy, 2)

    barrier = pltpu.get_barrier_semaphore()

    @pl.loop(1, devices)
    def _(step):
        there = lax.rem(flat + step, devices)
        pl.semaphore_signal(
            barrier,
            inc=1,
            device_id=(there // shard_count, lax.rem(there, shard_count)),
            device_id_type=MESH,
        )

    gain = gain_ref[...].astype(jnp.bfloat16).astype(jnp.float32)
    query = QHEADS * HEAD_DIM // TP
    pair = KVHEADS * HEAD_DIM // TP
    for rank in range(TP):
        starts = (
            (rank * query, 0, query),
            (TP * query + rank * pair, query, pair),
            (TP * (query + pair) + rank * pair, query + pair, pair),
        )
        for source, target, extent in starts:
            part = w_ref[:, source : source + extent].astype(jnp.bfloat16).astype(jnp.float32)
            wsend[rank, :, target : target + extent] = (part * gain).astype(jnp.bfloat16)
    for piece in range(pieces):
        tbuf[me * pieces + piece] = tok_ref[piece * piece_rows : (piece + 1) * piece_rows, :]
    bbuf[flat] = bias_ref[...]
    pl.semaphore_wait(barrier, devices - 1)

    def token_copy(block, piece, way, target):
        index = block * pieces + piece
        return pltpu.make_async_remote_copy(
            src_ref=tbuf.at[index],
            dst_ref=tbuf.at[index],
            send_sem=t_send.at[way, index],
            recv_sem=t_recv.at[index],
            device_id=(inst, target),
            device_id_type=MESH,
        )

    def own_token_copy(piece, way, target):
        index = me * pieces + piece
        return pltpu.make_async_remote_copy(
            src_ref=tok_ref.at[pl.ds(piece * piece_rows, piece_rows)],
            dst_ref=tbuf.at[index],
            send_sem=t_send.at[way, index],
            recv_sem=t_recv.at[index],
            device_id=(inst, target),
            device_id_type=MESH,
        )

    def weight_copy(source, target, slot, send_sem):
        return pltpu.make_async_remote_copy(
            src_ref=source,
            dst_ref=wbuf.at[slot],
            send_sem=send_sem,
            recv_sem=w_recv.at[slot],
            device_id=target,
            device_id_type=MESH,
        )

    def all_gather_copy(k):
        there = mate(k)
        return weight_copy(wsend.at[there], (inst, there), flat, a_send.at[k])

    def x_copy(k):
        slot = inst * shard_count + mate(k)
        source = wsend.at[me] if k == 0 else wbuf.at[slot]
        return weight_copy(source, (x_peer, me), slot, x_send.at[k])

    def core_copy(k, owner, side):
        slot = owner * shard_count + mate(k)
        source = wsend.at[me] if k == 0 and side == 0 else wbuf.at[slot]
        return weight_copy(source, (core_peer, me), slot, d_send.at[side, k])

    up = lax.rem(z + 1, line) * 2 + y
    down = lax.rem(z + line - 1, line) * 2 + y

    def each(condition, action):
        pl.when(condition)(action)

    for piece in range(pieces):
        each(z < line - 1, lambda piece=piece: own_token_copy(piece, 0, up).start())
        each(z > 0, lambda piece=piece: own_token_copy(piece, 1, down).start())
        own_token_copy(piece, 2, y_peer).start()
    core_copy(0, inst, 0).start()
    x_copy(0).start()
    order = (7, 6, 5, 4, 3, 2, 1)
    for k in order:
        all_gather_copy(k).start()

    def bias_copy(step):
        there = lax.rem(flat + step, devices)
        return pltpu.make_async_remote_copy(
            src_ref=bias_ref,
            dst_ref=bbuf.at[flat],
            send_sem=b_send.at[step],
            recv_sem=b_recv.at[flat],
            device_id=(there // shard_count, lax.rem(there, shard_count)),
            device_id_type=MESH,
        )

    @pl.loop(1, devices)
    def _(step):
        bias_copy(step).start()

    wbuf[flat] = wsend[me]

    def wait_block(slot):
        pltpu.make_async_copy(wbuf.at[slot], wbuf.at[slot], w_recv.at[slot]).wait()

    def wait_token(block, piece):
        index = block * pieces + piece
        pltpu.make_async_copy(tbuf.at[index], tbuf.at[index], t_recv.at[index]).wait()

    def relay_token(distance, piece):
        def from_below():
            block = (z - distance) * 2 + y
            wait_token(block, piece)
            each(z < line - 1, lambda: token_copy(block, piece, 0, up).start())
            token_copy(block, piece, 2, y_peer).start()

        def from_above():
            block = (z + distance) * 2 + y
            wait_token(block, piece)
            each(z > 0, lambda: token_copy(block, piece, 1, down).start())
            token_copy(block, piece, 2, y_peer).start()

        each(z >= distance, from_below)
        each(z + distance < line, from_above)

    def relay_weight(k):
        wait_block(inst * shard_count + mate(k))
        x_copy(k).start()
        core_copy(k, inst, 0).start()

    def relay_x(k):
        wait_block(x_peer * shard_count + mate(k))
        core_copy(k, x_peer, 1).start()

    def relay_hop(distance):
        for piece in range(pieces):
            relay_token(distance, piece)

    def scale_of(index):
        values = tbuf[index].astype(jnp.float32)
        mean = jnp.sum(values * values, axis=-1, keepdims=True) * (1.0 / tok_ref.shape[1])
        scale_ref[pl.ds(pl.multiple_of(index * piece_rows, piece_rows), piece_rows), :] = jnp.broadcast_to(
            lax.rsqrt(mean + EPSILON), (piece_rows, LANES)
        )

    relay_hop(1)
    relay_x(0)
    for k in order[:3]:
        relay_weight(k)
    relay_hop(2)
    for k in order[3:5]:
        relay_weight(k)
    for k in order[:2]:
        relay_x(k)
    relay_hop(3)
    for k in order[5:]:
        relay_weight(k)
    for k in order[2:]:
        relay_x(k)

    for k in range(shard_count):
        wait_block(core_peer * shard_count + mate(k))
        wait_block(lax.rem(core_peer + 2, inst_count) * shard_count + mate(k))
    for block_z in range(line):
        for piece in range(pieces):
            wait_token(block_z * 2 + 1 - y, piece)

    @pl.loop(0, shard_count * pieces)
    def _(index):
        scale_of(index)

    @pl.loop(1, devices)
    def _(step):
        slot = lax.rem(flat + step, devices)
        pltpu.make_async_copy(bbuf.at[slot], bbuf.at[slot], b_recv.at[slot]).wait()

    per_row = LANES // group
    held = bias_ref.shape[0]
    lane = lax.broadcasted_iota(jnp.int32, (1, LANES), 1) // group

    def bias_row(first):
        row = jnp.zeros((1, LANES), jnp.float32)
        for j in range(per_row):
            number = first + j
            row = jnp.where(lane == j, bbuf[number // held, pl.ds(lax.rem(number, held), 1), :], row)
        return row.astype(jnp.bfloat16).astype(jnp.float32)

    tile = 2 * LANES
    depth = devices * rows
    scale = scale_ref[...]
    for start in range(0, width, tile):
        extent = min(tile, width - start)
        product = jnp.dot(
            tbuf[...].reshape(shard_count * pieces * piece_rows, depth),
            wbuf[:, :, start : start + extent].reshape(depth, extent),
            preferred_element_type=jnp.float32,
        )
        for inner in range(0, extent, LANES):
            at = start + inner
            if at < query:
                column = me * query + at
            elif at < query + pair:
                column = TP * query + me * pair + (at - query)
            else:
                column = TP * (query + pair) + me * pair + (at - query - pair)
            out_ref[0, :, at : at + LANES] = (
                product[:, inner : inner + LANES] * scale + bias_row(column // group)
            ).astype(jnp.bfloat16)

    for piece in range(pieces):
        each(z < line - 1, lambda piece=piece: own_token_copy(piece, 0, up).wait_send())
        each(z > 0, lambda piece=piece: own_token_copy(piece, 1, down).wait_send())
        own_token_copy(piece, 2, y_peer).wait_send()
        for distance in range(1, line):

            def below(piece=piece, distance=distance):
                block = (z - distance) * 2 + y
                each(z < line - 1, lambda: token_copy(block, piece, 0, up).wait_send())
                token_copy(block, piece, 2, y_peer).wait_send()

            def above(piece=piece, distance=distance):
                block = (z + distance) * 2 + y
                each(z > 0, lambda: token_copy(block, piece, 1, down).wait_send())
                token_copy(block, piece, 2, y_peer).wait_send()

            each(z >= distance, below)
            each(z + distance < line, above)
    for k in range(shard_count):
        if k:
            all_gather_copy(k).wait_send()
        x_copy(k).wait_send()
        core_copy(k, inst, 0).wait_send()
        core_copy(k, x_peer, 1).wait_send()

    @pl.loop(1, devices)
    def _(step):
        bias_copy(step).wait_send()


def kernel_device(dims, tokens, norm_gain, master_qkv, qkv_bias):
    inst_count, shard_count, group = dims
    devices = inst_count * shard_count
    rows = master_qkv.shape[0]
    width = master_qkv.shape[1] // TP
    pieces = TOKEN_PIECES
    groups = qkv_bias.shape[0] // group
    bias = jnp.tile(qkv_bias.reshape(groups, group), (1, LANES // group))
    index_count = shard_count * pieces
    dma = pltpu.SemaphoreType.DMA
    vmem = pl.BlockSpec(memory_space=pltpu.VMEM)
    return pl.pallas_call(
        functools.partial(kernel, dims),
        out_shape=jax.ShapeDtypeStruct((1, shard_count * tokens.shape[0], width), jnp.bfloat16),
        in_specs=[vmem] * 4,
        out_specs=vmem,
        scratch_shapes=[
            pltpu.VMEM((index_count, tokens.shape[0] // pieces, tokens.shape[1]), jnp.bfloat16),
            pltpu.VMEM((devices, rows, width), jnp.bfloat16),
            pltpu.VMEM((TP, rows, width), jnp.bfloat16),
            pltpu.VMEM((devices, groups, LANES), jnp.float32),
            pltpu.VMEM((shard_count * tokens.shape[0], LANES), jnp.float32),
            dma((index_count,)),
            dma((3, index_count)),
            dma((devices,)),
            dma((shard_count,)),
            dma((shard_count,)),
            dma((2, shard_count)),
            dma((devices,)),
            dma((devices,)),
        ],
        compiler_params=pltpu.CompilerParams(
            collective_id=0, has_side_effects=True, vmem_limit_bytes=60 * 1024 * 1024
        ),
    )(tokens, norm_gain.reshape(rows, 1), master_qkv, bias)


def per_device(tokens, norm_gain, master_qkv, qkv_bias):
    inst_count, shard_count = lax.axis_size("inst"), lax.axis_size("shard")
    group = 32
    fits = (
        shard_count == TP
        and inst_count == 4
        and master_qkv.shape[0] % 16 == 0
        and tokens.shape[0] % (16 * TOKEN_PIECES) == 0
        and qkv_bias.shape[0] % group == 0
    )
    if fits:
        return kernel_device((inst_count, shard_count, group), tokens, norm_gain, master_qkv, qkv_bias)
    return general_device(tokens, norm_gain, master_qkv, qkv_bias)


def solution(mesh):
    in_specs = (
        P(("inst", "shard"), None),
        P(("inst", "shard")),
        P(("inst", "shard"), None),
        P(("inst", "shard")),
    )
    out_specs = P(("inst", "shard"), None, None)
    return jax.shard_map(
        per_device, mesh=mesh, in_specs=in_specs, out_specs=out_specs, check_vma=False
    )
```

```python
import functools

import jax
import jax.numpy as jnp
from jax import lax
from jax.experimental import pallas as pl
from jax.experimental.pallas import tpu as pltpu
from jax.sharding import PartitionSpec as P

QHEADS = 40
KVHEADS = 8
HEAD_DIM = 128
TP = 8


EPSILON = 1e-06
MESH = pl.DeviceIdType.MESH
LANES = 128
TOKEN_PIECES = 2


def partner_2(value, axis, distance):
    mask = 2**distance
    pairs = [(source, source ^ mask) for source in range(lax.axis_size(axis))]
    return lax.ppermute(value, axis, pairs)


def rank_columns(matrix):
    query_cols = QHEADS * HEAD_DIM
    pair_cols = KVHEADS * HEAD_DIM
    leading = matrix.shape[:-1]
    query = matrix[..., :query_cols].reshape(leading + (TP, query_cols // TP))
    keys = matrix[..., query_cols : query_cols + pair_cols].reshape(leading + (TP, pair_cols // TP))
    values = matrix[..., query_cols + pair_cols :].reshape(leading + (TP, pair_cols // TP))
    return jnp.concatenate([query, keys, values], axis=-1)


def normalize(tokens, gain):
    floats = tokens.astype(jnp.float32)
    scale = lax.rsqrt(jnp.mean(floats * floats, axis=-1, keepdims=True) + EPSILON)
    return (floats * scale * gain.astype(jnp.float32)).astype(jnp.bfloat16)


def general_device(tokens, norm_gain, master_qkv, qkv_bias):
    shard_count = lax.axis_size("shard")
    local_rows = master_qkv.shape[0]
    rank_width = master_qkv.shape[1] // TP
    gain_full, bias_full = (
        lax.all_gather(norm_gain.astype(jnp.bfloat16), ("inst", "shard"), axis=0, tiled=True),
        lax.all_gather(qkv_bias.astype(jnp.bfloat16), ("inst", "shard"), axis=0, tiled=True),
    )
    normed = normalize(tokens, gain_full)
    shard_pos = lax.axis_index("shard")
    rank_index = shard_pos % TP
    bit_count = TP.bit_length() - 1
    bit_order = list(range(bit_count))
    group_rows = normed
    for bit_pos in bit_order:
        partner = partner_2(group_rows, "shard", bit_pos)
        lower = jnp.bitwise_and(jnp.right_shift(shard_pos, bit_pos), 1) == 0
        group_rows = jnp.where(
            lower,
            jnp.concatenate([group_rows, partner], 0),
            jnp.concatenate([partner, group_rows], 0),
        )
    copies = shard_count // TP
    inst_block = shard_count * local_rows
    rows_low = master_qkv.astype(jnp.bfloat16)
    ranked = jnp.transpose(rank_columns(rows_low), (1, 0, 2))
    spread = jnp.broadcast_to(ranked[None], (copies,) + ranked.shape)
    outgoing = spread.reshape(shard_count, rows_low.shape[0], rank_width)
    arrived = lax.all_to_all(outgoing, "shard", split_axis=0, concat_axis=0, tiled=True).reshape(
        inst_block, rank_width
    )
    product = jnp.dot(
        group_rows,
        lax.all_gather(arrived, "inst", axis=0, tiled=True),
        preferred_element_type=jnp.float32,
    )
    bias_ranks = rank_columns(bias_full)
    bias_mine = lax.dynamic_index_in_dim(bias_ranks, rank_index, 0, keepdims=False)
    result = (product + bias_mine.astype(jnp.float32)).astype(jnp.bfloat16)
    return result[None]


def kernel(
    dims,
    tok_ref,
    gain_ref,
    w_ref,
    bias_ref,
    out_ref,
    tbuf,
    wbuf,
    wsend,
    bbuf,
    scale_ref,
    t_recv,
    t_send,
    w_recv,
    a_send,
    x_send,
    d_send,
    b_recv,
    b_send,
):
    inst_count, shard_count, group = dims
    devices = inst_count * shard_count
    line = shard_count // 2
    inst = lax.axis_index("inst")
    me = lax.axis_index("shard")
    z = me // 2
    y = lax.rem(me, 2)
    flat = inst * shard_count + me
    core_peer = inst + 1 - 2 * lax.rem(inst, 2)
    x_peer = lax.rem(inst + 2, inst_count)
    y_peer = z * 2 + 1 - y
    rows = w_ref.shape[0]
    width = wsend.shape[2]
    pieces = TOKEN_PIECES
    piece_rows = tok_ref.shape[0] // pieces

    def mate(k):
        dy, dz = k % 2, k // 2
        zz = z if dz == 0 else (z + 1 - 2 * lax.rem(z, 2), lax.rem(z + 2, line), line - 1 - z)[dz - 1]
        return zz * 2 + lax.rem(y + dy, 2)

    barrier = pltpu.get_barrier_semaphore()

    @pl.loop(1, devices)
    def _(step):
        there = lax.rem(flat + step, devices)
        pl.semaphore_signal(
            barrier,
            inc=1,
            device_id=(there // shard_count, lax.rem(there, shard_count)),
            device_id_type=MESH,
        )

    for piece in range(pieces):
        tbuf[me * pieces + piece] = tok_ref[piece * piece_rows : (piece + 1) * piece_rows, :]
    bbuf[flat] = bias_ref[...]
    pl.semaphore_wait(barrier, devices - 1)

    def token_copy(block, piece, way, target):
        index = block * pieces + piece
        return pltpu.make_async_remote_copy(
            src_ref=tbuf.at[index],
            dst_ref=tbuf.at[index],
            send_sem=t_send.at[way, index],
            recv_sem=t_recv.at[index],
            device_id=(inst, target),
            device_id_type=MESH,
        )

    def own_token_copy(piece, way, target):
        index = me * pieces + piece
        return pltpu.make_async_remote_copy(
            src_ref=tok_ref.at[pl.ds(piece * piece_rows, piece_rows)],
            dst_ref=tbuf.at[index],
            send_sem=t_send.at[way, index],
            recv_sem=t_recv.at[index],
            device_id=(inst, target),
            device_id_type=MESH,
        )

    def weight_copy(source, target, slot, send_sem):
        return pltpu.make_async_remote_copy(
            src_ref=source,
            dst_ref=wbuf.at[slot],
            send_sem=send_sem,
            recv_sem=w_recv.at[slot],
            device_id=target,
            device_id_type=MESH,
        )

    def all_gather_copy(k):
        there = mate(k)
        return weight_copy(wsend.at[there], (inst, there), flat, a_send.at[k])

    def x_copy(k):
        slot = inst * shard_count + mate(k)
        source = wsend.at[me] if k == 0 else wbuf.at[slot]
        return weight_copy(source, (x_peer, me), slot, x_send.at[k])

    def core_copy(k, owner, side):
        slot = owner * shard_count + mate(k)
        source = wsend.at[me] if k == 0 and side == 0 else wbuf.at[slot]
        return weight_copy(source, (core_peer, me), slot, d_send.at[side, k])

    up = lax.rem(z + 1, line) * 2 + y
    down = lax.rem(z + line - 1, line) * 2 + y

    def each(condition, action):
        pl.when(condition)(action)

    for piece in range(pieces):
        each(z < line - 1, lambda piece=piece: own_token_copy(piece, 0, up).start())
        each(z > 0, lambda piece=piece: own_token_copy(piece, 1, down).start())
        own_token_copy(piece, 2, y_peer).start()
    gain = gain_ref[...].astype(jnp.bfloat16).astype(jnp.float32)
    query = QHEADS * HEAD_DIM // TP
    pair = KVHEADS * HEAD_DIM // TP
    for rank in range(TP):
        starts = (
            (rank * query, 0, query),
            (TP * query + rank * pair, query, pair),
            (TP * (query + pair) + rank * pair, query + pair, pair),
        )
        for source, target, extent in starts:
            part = w_ref[:, source : source + extent].astype(jnp.bfloat16).astype(jnp.float32)
            wsend[rank, :, target : target + extent] = (part * gain).astype(jnp.bfloat16)
    core_copy(0, inst, 0).start()
    x_copy(0).start()
    all_gather_copy(1).start()
    all_gather_copy(2).start()
    all_gather_copy(3).start()

    def bias_copy(step):
        there = lax.rem(flat + step, devices)
        return pltpu.make_async_remote_copy(
            src_ref=bias_ref,
            dst_ref=bbuf.at[flat],
            send_sem=b_send.at[step],
            recv_sem=b_recv.at[flat],
            device_id=(there // shard_count, lax.rem(there, shard_count)),
            device_id_type=MESH,
        )

    @pl.loop(1, devices)
    def _(step):
        bias_copy(step).start()

    wbuf[flat] = wsend[me]

    def wait_block(slot):
        pltpu.make_async_copy(wbuf.at[slot], wbuf.at[slot], w_recv.at[slot]).wait()

    def wait_token(block, piece):
        index = block * pieces + piece
        pltpu.make_async_copy(tbuf.at[index], tbuf.at[index], t_recv.at[index]).wait()

    def relay_token(distance, piece):
        def from_below():
            block = (z - distance) * 2 + y
            wait_token(block, piece)
            each(z < line - 1, lambda: token_copy(block, piece, 0, up).start())
            token_copy(block, piece, 2, y_peer).start()

        def from_above():
            block = (z + distance) * 2 + y
            wait_token(block, piece)
            each(z > 0, lambda: token_copy(block, piece, 1, down).start())
            token_copy(block, piece, 2, y_peer).start()

        each(z >= distance, from_below)
        each(z + distance < line, from_above)

    def relay_weight(k):
        wait_block(inst * shard_count + mate(k))
        x_copy(k).start()
        core_copy(k, inst, 0).start()

    def relay_x(k):
        wait_block(x_peer * shard_count + mate(k))
        core_copy(k, x_peer, 1).start()

    def relay_hop(distance):
        for piece in range(pieces):
            relay_token(distance, piece)

    def scale_of(index):
        values = tbuf[index].astype(jnp.float32)
        mean = jnp.sum(values * values, axis=-1, keepdims=True) * (1.0 / tok_ref.shape[1])
        scale_ref[pl.ds(pl.multiple_of(index * piece_rows, piece_rows), piece_rows), :] = jnp.broadcast_to(
            lax.rsqrt(mean + EPSILON), (piece_rows, LANES)
        )

    relay_hop(1)
    all_gather_copy(4).start()
    all_gather_copy(5).start()
    all_gather_copy(6).start()
    all_gather_copy(7).start()
    relay_x(0)
    relay_weight(1)
    relay_weight(2)
    relay_weight(3)
    relay_hop(2)
    relay_weight(4)
    relay_weight(5)
    relay_hop(3)
    relay_x(1)
    relay_x(2)
    relay_weight(6)
    relay_weight(7)
    relay_x(3)
    relay_x(4)
    relay_x(5)
    relay_x(6)
    relay_x(7)

    for k in range(shard_count):
        wait_block(core_peer * shard_count + mate(k))
        wait_block(lax.rem(core_peer + 2, inst_count) * shard_count + mate(k))
    for block_z in range(line):
        for piece in range(pieces):
            wait_token(block_z * 2 + 1 - y, piece)

    @pl.loop(0, shard_count * pieces)
    def _(index):
        scale_of(index)

    @pl.loop(1, devices)
    def _(step):
        slot = lax.rem(flat + step, devices)
        pltpu.make_async_copy(bbuf.at[slot], bbuf.at[slot], b_recv.at[slot]).wait()

    per_row = LANES // group
    held = bias_ref.shape[0]
    lane = lax.broadcasted_iota(jnp.int32, (1, LANES), 1) // group

    def bias_row(first):
        row = jnp.zeros((1, LANES), jnp.float32)
        for j in range(per_row):
            number = first + j
            row = jnp.where(lane == j, bbuf[number // held, pl.ds(lax.rem(number, held), 1), :], row)
        return row.astype(jnp.bfloat16).astype(jnp.float32)

    tile = 2 * LANES
    depth = devices * rows
    scale = scale_ref[...]
    for start in range(0, width, tile):
        extent = min(tile, width - start)
        product = jnp.dot(
            tbuf[...].reshape(shard_count * pieces * piece_rows, depth),
            wbuf[:, :, start : start + extent].reshape(depth, extent),
            preferred_element_type=jnp.float32,
        )
        for inner in range(0, extent, LANES):
            at = start + inner
            if at < query:
                column = me * query + at
            elif at < query + pair:
                column = TP * query + me * pair + (at - query)
            else:
                column = TP * (query + pair) + me * pair + (at - query - pair)
            out_ref[0, :, at : at + LANES] = (
                product[:, inner : inner + LANES] * scale + bias_row(column // group)
            ).astype(jnp.bfloat16)

    for piece in range(pieces):
        each(z < line - 1, lambda piece=piece: own_token_copy(piece, 0, up).wait_send())
        each(z > 0, lambda piece=piece: own_token_copy(piece, 1, down).wait_send())
        own_token_copy(piece, 2, y_peer).wait_send()
        for distance in range(1, line):

            def below(piece=piece, distance=distance):
                block = (z - distance) * 2 + y
                each(z < line - 1, lambda: token_copy(block, piece, 0, up).wait_send())
                token_copy(block, piece, 2, y_peer).wait_send()

            def above(piece=piece, distance=distance):
                block = (z + distance) * 2 + y
                each(z > 0, lambda: token_copy(block, piece, 1, down).wait_send())
                token_copy(block, piece, 2, y_peer).wait_send()

            each(z >= distance, below)
            each(z + distance < line, above)
    for k in range(shard_count):
        if k:
            all_gather_copy(k).wait_send()
        x_copy(k).wait_send()
        core_copy(k, inst, 0).wait_send()
        core_copy(k, x_peer, 1).wait_send()

    @pl.loop(1, devices)
    def _(step):
        bias_copy(step).wait_send()


def kernel_device(dims, tokens, norm_gain, master_qkv, qkv_bias):
    inst_count, shard_count, group = dims
    devices = inst_count * shard_count
    rows = master_qkv.shape[0]
    width = master_qkv.shape[1] // TP
    pieces = TOKEN_PIECES
    groups = qkv_bias.shape[0] // group
    bias = jnp.tile(qkv_bias.reshape(groups, group), (1, LANES // group))
    index_count = shard_count * pieces
    dma = pltpu.SemaphoreType.DMA
    vmem = pl.BlockSpec(memory_space=pltpu.VMEM)
    return pl.pallas_call(
        functools.partial(kernel, dims),
        out_shape=jax.ShapeDtypeStruct((1, shard_count * tokens.shape[0], width), jnp.bfloat16),
        in_specs=[vmem] * 4,
        out_specs=vmem,
        scratch_shapes=[
            pltpu.VMEM((index_count, tokens.shape[0] // pieces, tokens.shape[1]), jnp.bfloat16),
            pltpu.VMEM((devices, rows, width), jnp.bfloat16),
            pltpu.VMEM((TP, rows, width), jnp.bfloat16),
            pltpu.VMEM((devices, groups, LANES), jnp.float32),
            pltpu.VMEM((shard_count * tokens.shape[0], LANES), jnp.float32),
            dma((index_count,)),
            dma((3, index_count)),
            dma((devices,)),
            dma((shard_count,)),
            dma((shard_count,)),
            dma((2, shard_count)),
            dma((devices,)),
            dma((devices,)),
        ],
        compiler_params=pltpu.CompilerParams(
            collective_id=0, has_side_effects=True, vmem_limit_bytes=60 * 1024 * 1024
        ),
    )(tokens, norm_gain.reshape(rows, 1), master_qkv, bias)


def per_device(tokens, norm_gain, master_qkv, qkv_bias):
    inst_count, shard_count = lax.axis_size("inst"), lax.axis_size("shard")
    group = 32
    fits = (
        shard_count == TP
        and inst_count == 4
        and master_qkv.shape[0] % 16 == 0
        and tokens.shape[0] % (16 * TOKEN_PIECES) == 0
        and qkv_bias.shape[0] % group == 0
    )
    if fits:
        return kernel_device((inst_count, shard_count, group), tokens, norm_gain, master_qkv, qkv_bias)
    return general_device(tokens, norm_gain, master_qkv, qkv_bias)


def solution(mesh):
    in_specs = (
        P(("inst", "shard"), None),
        P(("inst", "shard")),
        P(("inst", "shard"), None),
        P(("inst", "shard")),
    )
    out_specs = P(("inst", "shard"), None, None)
    return jax.shard_map(
        per_device, mesh=mesh, in_specs=in_specs, out_specs=out_specs, check_vma=False
    )
```
